32 devices in a mesh: dp: 2 (over x), expert: 4 (over z), mp: 4 (over y, core).
Axes of the slice: x: 2, y: 2, z: 4, core: 2. Of those that a mesh axis runs over, the one named last changes fastest.
Arguments:
- tokens: bfloat16 [128, 4096], P(('dp', 'expert', 'mp')), may hold values from -6 to 6
- probes: bfloat16 [2, 128, 4096], P(None, ('dp', 'expert', 'mp')), may hold values from -6 to 6
- cotangent: bfloat16 [128, 4096], P(('dp', 'expert', 'mp')), may hold values from -0.119628906 to 0.119628906
- expert_ids: int32 [128, 2], P(('dp', 'expert', 'mp')), may hold values from 0 to 3, all different within a row; in each aligned block of 4 rows (0 to 3, 4 to 7, ...) at most 4 rows name the same one
- combine: float32 [128, 2], P(('dp', 'expert', 'mp')), may hold values from 0.2 to 1
- w_gate: bfloat16 [4, 4096, 14336], P('expert', None, ('dp', 'mp')), may hold values from -0.09375 to 0.09375
- w_up: bfloat16 [4, 4096, 14336], P('expert', None, ('dp', 'mp')), may hold values from -0.09375 to 0.09375
- w_down: bfloat16 [4, 14336, 4096], P('expert', ('dp', 'mp')), may hold values from -0.046875 to 0.046875
Outputs:
- quad: float32 [2, 128], P(None, ('dp', 'expert', 'mp'))
The draws below stay inside these ranges and needn't reach their ends.
Inputs may be any that keep to these rules, and one draw needn't show every extreme that they name: `expert_ids`: each token names 2 different experts. In each aligned block of 4 tokens (the tokens of one device) no expert is named by more than 4 of them, and some block reaches 4.
All inputs are finite; a program needn't handle non-finite values.
Results may differ from the reference program's by a relative error of at most 0.003.
Values may be sent and summed in bfloat16 or wider, within the bound.
No kernel may reach another device: no remote copies, remote signals or barrier semaphores. Data moves between devices by JAX's collectives and lax.ppermute only.
A program may use at most 128 MiB of HBM per device.

```python
import math
import jax
import jax.numpy as jnp
import numpy as np
from jax import lax

D = 4096
FF = 14336
TOP = 2
PROBES = 2
TOK_DEV = 4
EXPERTS = 4
CAP = 4
TOKENS = 128


def block_levels(stream_key, extent, shards, smallest, largest):
    loudness, own = 1.0, jax.random.fold_in(stream_key, 6)
    for dim, shards_of in shards:
        heights = jnp.exp(jax.random.uniform(jax.random.fold_in(own, dim), (shards_of,), jnp.float32, smallest / len(shards), largest / len(shards)))
        loudness = loudness * jnp.repeat(heights, extent[dim] // shards_of).reshape([-1 if axis == dim else 1 for axis in range(len(extent))])
    return loudness


def deal_out(own_key, own, number, rows, number_of, top, limit, lean):
    sequence = jax.random.permutation(own_key, number_of)
    crowded, usual = load_shares(number_of, rows * top, limit, lean, True), load_shares(number_of, rows * top, limit, lean, False)
    places = jnp.arange(number_of)

    def named(lengths, offset_by):
        used = int((lengths > 0).sum())
        fixed = max(1, used // 4)
        moved = fixed + (places - fixed + offset_by * (used - fixed)) % max(1, number_of - fixed)
        return jnp.zeros((number_of,), jnp.int32).at[sequence[jnp.where(places < fixed, places, moved)]].set(jnp.asarray(lengths, jnp.int32))

    lengths = jnp.where(number % 4 == 0, named(crowded, number // 4), named(usual, number - number // 4 - 1))
    mixed = jax.random.permutation(jax.random.fold_in(own, 3), number_of)
    giver, receiver = mixed[0:number_of // 2 * 2:2], mixed[1:number_of // 2 * 2:2]
    room = jnp.minimum(lengths[giver] - 1, limit - lengths[receiver]) // 2
    room = jnp.where((giver == sequence[0]) | (receiver == sequence[0]) | (lengths[receiver] == 0), 0, jnp.maximum(room, 0))
    moved = jax.random.randint(jax.random.fold_in(own, 4), (number_of // 2,), 0, 1 << 20) % (room + 1)
    lengths = lengths.at[giver].add(-moved).at[receiver].add(moved)
    items = jnp.searchsorted(jnp.cumsum(lengths), jnp.arange(rows * top), side="right").astype(jnp.int32)
    table = items.reshape(top, rows).T
    table = table[jax.random.permutation(jax.random.fold_in(own, 1), rows)]
    offset_by = jax.random.randint(jax.random.fold_in(own, 2), (rows, 1), 0, top)
    return jnp.take_along_axis(table, (jnp.arange(top)[None, :] + offset_by) % top, axis=1)


def load_shares(amount, total, limit, slope, full):
    portions = [(1 << 20) // math.isqrt(grade ** slope) + 1 for grade in range(1, amount + 1)]
    largest = limit if full else min(limit, max(-(-total // amount), total * portions[0] // sum(portions)))
    least = 1 if total - largest >= amount - 1 else 0
    given, rest = [largest] + [least] * (amount - 1), total - largest - least * (amount - 1)
    while rest > 0:
        free = [i for i in range(1, amount) if given[i] < largest] or [i for i in range(1, amount) if given[i] < limit]
        pool, budget = sum([portions[i] for i in free]), rest
        for i in free:
            more = min(limit - given[i], max(1, budget * portions[i] // pool), rest)
            given[i] = given[i] + more
            rest = rest - more
    return np.array(given)


def scatter_about(rng, shape, scale, limit, cuts=(), kind=jnp.bfloat16):
    gain = block_levels(rng, shape, cuts, -0.22, 0.18) if cuts else 1.0
    drawn = jax.random.normal(rng, shape, jnp.float32) * scale * gain
    return jnp.minimum(jnp.maximum(drawn, -limit), limit).astype(kind)


def setup_inputs(seed: int = 0) -> dict:
    seeds = jax.random.split(jax.random.key(seed), 9)
    tokens = scatter_about(seeds[0], (TOKENS, D), 1.0, 6.0, ((0, 32),))
    probes = scatter_about(seeds[1], (PROBES, TOKENS, D), 1.0, 6.0, ((1, 32),))
    cotangent = scatter_about(seeds[2], (TOKENS, D), 0.02, 0.119628906, ((0, 32),))
    expert_ids_keys = jax.random.split(jax.random.fold_in(seeds[3], 1), TOKENS // TOK_DEV)
    expert_ids_turns = jax.random.permutation(jax.random.fold_in(seeds[3], 3), TOKENS // TOK_DEV)
    expert_ids = jax.vmap(lambda own, number: deal_out(jax.random.fold_in(seeds[3], 2), own, number, TOK_DEV, EXPERTS, TOP, CAP, 2))(expert_ids_keys, expert_ids_turns).reshape((TOKENS, TOP))
    combine = jnp.clip(jnp.exp(math.log(1.0) - 1.609438 * jax.random.uniform(seeds[4], (TOKENS, TOP), jnp.float32) ** block_levels(seeds[4], (TOKENS, TOP), ((0, 32),), -0.2, 0.2)), 0.2, 1.0)
    w_gate = scatter_about(seeds[5], (EXPERTS, D, FF), D ** -0.5, 0.09375, ((0, 4), (2, 8)))
    w_up = scatter_about(seeds[6], (EXPERTS, D, FF), D ** -0.5, 0.09375, ((0, 4), (2, 8)))
    w_down = scatter_about(seeds[7], (EXPERTS, FF, D), FF ** -0.5, 0.046875, ((0, 4), (1, 8)))
    return {"tokens": tokens, "probes": probes, "cotangent": cotangent, "expert_ids": expert_ids, "combine": combine, "w_gate": w_gate, "w_up": w_up, "w_down": w_down}


def silu_slopes(preact):
    squash = jax.nn.sigmoid(preact)
    first_slope = squash * (1.0 + preact * (1.0 - squash))
    second_slope = squash * (1.0 - squash) * (2.0 + preact * (1.0 - 2.0 * squash))
    return first_slope, second_slope


def reference(tokens, probes, cotangent, expert_ids, combine, w_gate, w_up, w_down):
    def per_expert(carry, packed):
        expert_index, gate_weight, up_weight, down_weight = packed
        chosen = expert_ids == expert_index
        weight = jnp.sum(jnp.where(chosen, combine, jnp.zeros_like(combine)), axis=1)
        scaled = (weight[:, None] * cotangent.astype(jnp.float32)).astype(jnp.bfloat16)
        gate_pre = jnp.dot(tokens, gate_weight, preferred_element_type=jnp.float32)
        up_pre = jnp.dot(tokens, up_weight, preferred_element_type=jnp.float32)
        readout = lax.dot_general(scaled, down_weight, (((1,), (1,)), ((), ())), preferred_element_type=jnp.float32)
        first_slope, second_slope = silu_slopes(gate_pre)

        def per_probe(direction):
            gate_tan = jnp.dot(direction, gate_weight, preferred_element_type=jnp.float32)
            up_tan = jnp.dot(direction, up_weight, preferred_element_type=jnp.float32)
            curved = second_slope * gate_tan * gate_tan * up_pre + 2.0 * first_slope * gate_tan * up_tan
            return jnp.sum(curved * readout, axis=1)

        return carry + lax.map(per_probe, probes), None

    start = jnp.zeros((PROBES, TOKENS), jnp.float32)
    quad, _ = lax.scan(per_expert, start, (jnp.arange(EXPERTS, dtype=jnp.int32), w_gate, w_up, w_down))
    return quad
```

```python
import jax
import jax.numpy as jnp
import numpy as np
from jax import lax
from jax.experimental import pallas as pl
from jax.experimental.pallas import tpu as pltpu
from jax.sharding import Mesh
from jax.sharding import PartitionSpec as P

LANES = 128
FF_TILE = 256
KINDS = 4
VMEM_ROWS = 16 * 1024 * 1024


def silu_slopes(preact):
    squash = jax.nn.sigmoid(preact)
    first_slope = squash * (1.0 + preact * (1.0 - squash))
    second_slope = squash * (1.0 - squash) * (2.0 + preact * (1.0 - 2.0 * squash))
    return (first_slope, second_slope)


def routed_on_device(tokens, probes, cotangent, expert_ids, combine, w_gate, w_up, w_down):
    tok_dev, model_width = tokens.shape
    probe_count = probes.shape[0]
    top_count = expert_ids.shape[1]
    experts = lax.axis_size("expert") * w_gate.shape[0]
    capacity = 2 * max(1, tok_dev * top_count // experts)
    routed = tok_dev * top_count
    flat_ids = expert_ids.reshape(routed)
    positions = jnp.arange(routed, dtype=jnp.int32)
    same_expert = flat_ids[:, None] == flat_ids[None, :]
    before = positions[None, :] < positions[:, None]
    slot_index = jnp.sum((same_expert & before).astype(jnp.int32), axis=1)
    expert_hot = flat_ids[:, None] == jnp.arange(experts, dtype=jnp.int32)[None, :]
    slot_hot = slot_index[:, None] == jnp.arange(capacity, dtype=jnp.int32)[None, :]
    placing = (expert_hot[:, :, None] & slot_hot[:, None, :]).reshape(routed, experts * capacity)
    scaled = (
        combine.reshape(routed, 1) * jnp.repeat(cotangent.astype(jnp.float32), top_count, axis=0)
    ).astype(jnp.bfloat16)
    stacked = jnp.repeat(jnp.concatenate([tokens[None], probes], axis=0), top_count, axis=1)
    stacked = jnp.concatenate([stacked, scaled[None]], axis=0)
    outgoing = jnp.einsum(
        "nk,rnd->rkd", placing.astype(jnp.bfloat16), stacked, preferred_element_type=jnp.float32
    ).astype(jnp.bfloat16)
    outgoing = outgoing.reshape(probe_count + 2, experts, capacity, model_width)
    arrived = lax.all_to_all(outgoing, "expert", split_axis=1, concat_axis=1, tiled=True)
    arrived = arrived.reshape(probe_count + 2, experts * capacity, model_width)
    gate_local = w_gate[0]
    up_local = w_up[0]
    down_local = w_down[0]
    block_rows = lax.all_gather(arrived, ("dp", "mp"), axis=1, tiled=True)
    row_count = block_rows.shape[1]
    base_rows = block_rows[0]
    tangent = block_rows[1 : probe_count + 1].reshape(probe_count * row_count, model_width)
    readout_rows = block_rows[probe_count + 1]
    gate_pre = jnp.dot(base_rows, gate_local, preferred_element_type=jnp.float32)
    up_pre = jnp.dot(base_rows, up_local, preferred_element_type=jnp.float32)
    readout = lax.dot_general(
        readout_rows, down_local, (((1,), (1,)), ((), ())), preferred_element_type=jnp.float32
    )
    gate_tan = jnp.dot(tangent, gate_local, preferred_element_type=jnp.float32).reshape(
        probe_count, row_count, -1
    )
    up_tan = jnp.dot(tangent, up_local, preferred_element_type=jnp.float32).reshape(
        probe_count, row_count, -1
    )
    first_slope, second_slope = silu_slopes(gate_pre)
    curved = second_slope * gate_tan * gate_tan * up_pre + 2.0 * first_slope * gate_tan * up_tan
    partial_quad = jnp.sum(curved * readout, axis=2)
    spread = partial_quad.reshape(probe_count, -1, experts, capacity)
    swapped = lax.all_to_all(spread, "expert", split_axis=2, concat_axis=2, tiled=True)
    returned_table = lax.psum_scatter(swapped, ("dp", "mp"), scatter_dimension=1, tiled=True)
    returned_table = returned_table.reshape(probe_count, experts * capacity)
    per_choice = jnp.dot(
        returned_table, placing.astype(jnp.float32).T, precision=lax.Precision.HIGHEST
    )
    return jnp.sum(per_choice.reshape(probe_count, tok_dev, top_count), axis=2)


class Layout:
    def __init__(self, mesh):
        self.dp = mesh.shape["dp"]
        self.expert = mesh.shape["expert"]
        self.core = 2
        self.y = mesh.shape["mp"] // self.core
        self.count = mesh.size

    def pairs(self, dx, dz, dy, dc):
        out = []
        for x in range(self.dp):
            for z in range(self.expert):
                for y in range(self.y):
                    for c in range(self.core):
                        src = self.index(x, z, y, c)
                        dst = self.index(
                            (x + dx) % self.dp,
                            (z + dz) % self.expert,
                            (y + dy) % self.y,
                            (c + dc) % self.core,
                        )
                        out.append((src, dst))
        return out

    def index(self, x, z, y, c):
        return ((x * self.expert + z) * self.y + y) * self.core + c


AXES = ("dp", "expert", "mp")


def make_fast(mesh, lay):
    z_shifts = [0] + [k for k in range(1, lay.expert)]
    plane_shifts = [(dx, dy) for dx in range(lay.dp) for dy in range(lay.y)]
    offsets = [(dx, dz, dy) for (dx, dy) in plane_shifts for dz in z_shifts]

    def send(block, dx, dz, dy, dc):
        if dx == dz == dy == dc == 0:
            return block
        return lax.ppermute(block, AXES, lay.pairs(dx, dz, dy, dc))

    def gather(block):
        column = jnp.concatenate([send(block, 0, dz, 0, 0) for dz in z_shifts], axis=0)
        mine = jnp.concatenate([send(column, dx, 0, dy, 0) for dx, dy in plane_shifts], axis=0)
        return mine, send(mine, 0, 0, 0, 1)

    def pack(tokens, probes, cotangent, expert_ids, combine):
        tok_dev, width = tokens.shape
        rows = jnp.concatenate([tokens[None], probes, cotangent[None]], axis=0)
        rows = rows.reshape(KINDS * tok_dev, width)
        high = lax.reduce_precision(combine, 8, 7)
        rest = combine - high
        mid = lax.reduce_precision(rest, 8, 7)
        low = rest - mid
        meta = jnp.concatenate([expert_ids.astype(jnp.float32), high, mid, low], axis=1)
        meta = jnp.pad(meta, ((0, rows.shape[0] - tok_dev), (0, LANES - meta.shape[1])))
        return jnp.concatenate([rows, meta.astype(jnp.bfloat16)], axis=1)

    def on_device(tokens, probes, cotangent, expert_ids, combine, w_gate, w_up, w_down):
        tok_dev, width = tokens.shape
        top = expert_ids.shape[1]
        block = pack(tokens, probes, cotangent, expert_ids, combine)[None]
        mine, other = gather(block)
        partial = contract(mine, other, w_gate[0], w_up[0], w_down[0], tok_dev, top)
        swapped = lax.all_to_all(partial, AXES, split_axis=0, concat_axis=0, tiled=True)
        total = jnp.sum(swapped, axis=0)
        return total[: probes.shape[0] * tok_dev].reshape(probes.shape[0], tok_dev)

    def contract(mine, other, w_gate, w_up, w_down, tok_dev, top):
        half = mine.shape[0]
        width = w_gate.shape[0]
        ff = w_gate.shape[1]
        tiles = ff // FF_TILE
        rows = 2 * half * tok_dev
        group = 16 // tok_dev
        col = 512
        probe_count = KINDS - 2

        def body(mine_ref, other_ref, wg, wu, wd, out_ref, lhs, wts, meta, gbuf, ubuf, dbuf, acc, sems):
            def copies(i, slot):
                at = pl.multiple_of(i * FF_TILE, FF_TILE)
                return (
                    pltpu.make_async_copy(wg.at[:, pl.ds(at, FF_TILE)], gbuf.at[slot], sems.at[0, slot]),
                    pltpu.make_async_copy(wu.at[:, pl.ds(at, FF_TILE)], ubuf.at[slot], sems.at[1, slot]),
                    pltpu.make_async_copy(wd.at[pl.ds(at, FF_TILE), :], dbuf.at[slot], sems.at[2, slot]),
                )

            for slot in range(2):
                for c in copies(slot, slot):
                    c.start()

            upper = lax.broadcasted_iota(jnp.int32, (8, LANES), 0) < tok_dev

            def split(ref, g, at, size):
                pieces = [[] for _ in range(KINDS)]
                mask = lax.broadcasted_iota(jnp.int32, (8, size), 0) < tok_dev
                for pair in range(group // 2):
                    a = ref[g + 2 * pair, :, pl.ds(at, size)].astype(jnp.float32)
                    b = ref[g + 2 * pair + 1, :, pl.ds(at, size)].astype(jnp.float32)
                    for h in range(2):
                        ah = a[8 * h : 8 * h + 8]
                        bh = b[8 * h : 8 * h + 8]
                        pieces[2 * h].append(jnp.where(mask, ah, pltpu.roll(bh, tok_dev, 0)))
                        pieces[2 * h + 1].append(jnp.where(mask, pltpu.roll(ah, tok_dev, 0), bh))
                return [jnp.concatenate(p, axis=0) for p in pieces]

            expert = lax.axis_index("expert").astype(jnp.float32)
            for n, ref in enumerate((mine_ref, other_ref)):
                def take(i, _, n=n, ref=ref):
                    base = pl.multiple_of((n * half + i * group) * tok_dev, 16)
                    tags = split(ref, i * group, width, LANES)[0]
                    weight = jnp.zeros((16, 1), jnp.float32)
                    for j in range(top):
                        value = tags[:, top + j : top + j + 1] + tags[:, 2 * top + j : 2 * top + j + 1]
                        value = value + tags[:, 3 * top + j : 3 * top + j + 1]
                        weight = weight + jnp.where(tags[:, j : j + 1] == expert, value, 0.0)
                    for k in range(width // col):
                        parts = split(ref, i * group, k * col, col)
                        for kind in range(KINDS - 1):
                            lhs[pl.ds(kind * rows + base, 16), pl.ds(k * col, col)] = parts[kind].astype(jnp.bfloat16)
                        lhs[pl.ds((KINDS - 1) * rows + base, 16), pl.ds(k * col, col)] = (
                            weight * parts[KINDS - 1]
                        ).astype(jnp.bfloat16)
                    return 0

                lax.fori_loop(0, half // group, take, 0)

            acc[...] = jnp.zeros(acc.shape, jnp.float32)

            def tile(i, _):
                slot = lax.rem(i, 2)
                for c in copies(i, slot):
                    c.wait()
                split_at = (KINDS - 1) * rows
                gate = jnp.dot(lhs[:split_at, :], gbuf[slot], preferred_element_type=jnp.float32)
                up = jnp.dot(lhs[:split_at, :], ubuf[slot], preferred_element_type=jnp.float32)
                read = lax.dot_general(
                    lhs[split_at:, :], dbuf[slot], (((1,), (1,)), ((), ())), preferred_element_type=jnp.float32
                )

                @pl.when(i + 2 < tiles)
                def _():
                    for c in copies(i + 2, slot):
                        c.start()

                first, second = silu_slopes(gate[:rows])
                second = second * up[:rows] * read
                first = 2.0 * first * read
                for p in range(probe_count):
                    gate_tan = gate[(p + 1) * rows : (p + 2) * rows]
                    up_tan = up[(p + 1) * rows : (p + 2) * rows]
                    term = gate_tan * (second * gate_tan + first * up_tan)
                    for h in range(FF_TILE // LANES):
                        acc[p] += term[:, h * LANES : (h + 1) * LANES]
                return 0

            lax.fori_loop(0, tiles, tile, 0)

            def device_of(block):
                x = lax.axis_index("dp")
                z = lax.axis_index("expert")
                m = lax.axis_index("mp")
                y = m // lay.core
                c = m % lay.core
                out = jnp.zeros(block.shape, jnp.int32)
                for j, (dx, dz, dy) in enumerate(offsets):
                    for dc in range(lay.core):
                        src = lay.index(
                            (x + lay.dp - dx) % lay.dp,
                            (z + lay.expert - dz) % lay.expert,
                            (y + lay.y - dy) % lay.y,
                            (c + lay.core - dc) % lay.core,
                        )
                        out = jnp.where(block == dc * half + j, src, out)
                return out

            row_block = lax.broadcasted_iota(jnp.int32, (2 * half, rows), 1) // tok_dev
            hot = device_of(row_block) == lax.broadcasted_iota(jnp.int32, (2 * half, rows), 0)
            row = lax.broadcasted_iota(jnp.int32, (rows, LANES), 0) % tok_dev
            lane = lax.broadcasted_iota(jnp.int32, (rows, LANES), 1)
            spread = jnp.zeros((rows, LANES), jnp.float32)
            for p in range(probe_count):
                value = jnp.sum(acc[p], axis=1, keepdims=True)
                spread = spread + jnp.where(lane == row + p * tok_dev, value, 0.0)
            out_ref[...] = jnp.dot(
                hot.astype(jnp.float32), spread, precision=lax.Precision.HIGHEST, preferred_element_type=jnp.float32
            )

        vmem = pl.BlockSpec(memory_space=pltpu.VMEM)
        hbm = pl.BlockSpec(memory_space=pl.ANY)
        return pl.pallas_call(
            body,
            out_shape=jax.ShapeDtypeStruct((2 * half, LANES), jnp.float32),
            in_specs=[vmem, vmem, hbm, hbm, hbm],
            out_specs=vmem,
            scratch_shapes=[
                pltpu.VMEM((KINDS * rows, width), jnp.bfloat16),
                pltpu.VMEM((8, LANES), jnp.float32),
                pltpu.VMEM((8, LANES), jnp.float32),
                pltpu.VMEM((2, width, FF_TILE), jnp.bfloat16),
                pltpu.VMEM((2, width, FF_TILE), jnp.bfloat16),
                pltpu.VMEM((2, FF_TILE, width), jnp.bfloat16),
                pltpu.VMEM((probe_count, rows, LANES), jnp.float32),
                pltpu.SemaphoreType.DMA((3, 2)),
            ],
            compiler_params=pltpu.CompilerParams(vmem_limit_bytes=40 * 1024 * 1024),
            name="contract",
        )(mine, other, w_gate, w_up, w_down)

    return on_device


def fits(mesh, args):
    tokens, probes, w_gate = args[0], args[1], args[5]
    rows = (probes.shape[0] + 2) * tokens.shape[0]
    tok_dev = tokens.shape[0] // mesh.size
    return (
        mesh.shape["mp"] % 2 == 0
        and w_gate.shape[0] == mesh.shape["expert"]
        and probes.shape[0] + 2 == KINDS
        and tok_dev == 4
        and 4 * rows * tokens.shape[1] <= VMEM_ROWS
        and w_gate.shape[2] % (mesh.shape["dp"] * mesh.shape["mp"] * FF_TILE) == 0
    )


def solution(mesh):
    in_specs = (
        P(("dp", "expert", "mp"), None),
        P(None, ("dp", "expert", "mp"), None),
        P(("dp", "expert", "mp"), None),
        P(("dp", "expert", "mp"), None),
        P(("dp", "expert", "mp"), None),
        P("expert", None, ("dp", "mp")),
        P("expert", None, ("dp", "mp")),
        P("expert", ("dp", "mp"), None),
    )
    out_specs = P(None, ("dp", "expert", "mp"))

    def program(*args):
        body = make_fast(mesh, Layout(mesh)) if fits(mesh, args) else routed_on_device
        return jax.shard_map(
            body, mesh=mesh, in_specs=in_specs, out_specs=out_specs, check_vma=False
        )(*args)

    return program
```

```python
import jax
import jax.numpy as jnp
from jax import lax
from jax.experimental import pallas as pl
from jax.experimental.pallas import tpu as pltpu
from jax.sharding import PartitionSpec as P


LANES = 128
FF_TILE = 256
COLUMNS = 256
CUT = 22
SLOTS = 3
KINDS = 4
VMEM_ROWS = 16 * 1024 * 1024


def silu_slopes(preact):
    squash = jax.nn.sigmoid(preact)
    first_slope = squash * (1.0 + preact * (1.0 - squash))
    second_slope = squash * (1.0 - squash) * (2.0 + preact * (1.0 - 2.0 * squash))
    return (first_slope, second_slope)


def routed_on_device(tokens, probes, cotangent, expert_ids, combine, w_gate, w_up, w_down):
    tok_dev, model_width = tokens.shape
    probe_count = probes.shape[0]
    top_count = expert_ids.shape[1]
    experts = lax.axis_size("expert") * w_gate.shape[0]
    capacity = 2 * max(1, tok_dev * top_count // experts)
    routed = tok_dev * top_count
    flat_ids = expert_ids.reshape(routed)
    positions = jnp.arange(routed, dtype=jnp.int32)
    same_expert = flat_ids[:, None] == flat_ids[None, :]
    before = positions[None, :] < positions[:, None]
    slot_index = jnp.sum((same_expert & before).astype(jnp.int32), axis=1)
    expert_hot = flat_ids[:, None] == jnp.arange(experts, dtype=jnp.int32)[None, :]
    slot_hot = slot_index[:, None] == jnp.arange(capacity, dtype=jnp.int32)[None, :]
    placing = (expert_hot[:, :, None] & slot_hot[:, None, :]).reshape(routed, experts * capacity)
    scaled = (
        combine.reshape(routed, 1) * jnp.repeat(cotangent.astype(jnp.float32), top_count, axis=0)
    ).astype(jnp.bfloat16)
    stacked = jnp.repeat(jnp.concatenate([tokens[None], probes], axis=0), top_count, axis=1)
    stacked = jnp.concatenate([stacked, scaled[None]], axis=0)
    outgoing = jnp.einsum(
        "nk,rnd->rkd", placing.astype(jnp.bfloat16), stacked, preferred_element_type=jnp.float32
    ).astype(jnp.bfloat16)
    outgoing = outgoing.reshape(probe_count + 2, experts, capacity, model_width)
    arrived = lax.all_to_all(outgoing, "expert", split_axis=1, concat_axis=1, tiled=True)
    arrived = arrived.reshape(probe_count + 2, experts * capacity, model_width)
    gate_local = w_gate[0]
    up_local = w_up[0]
    down_local = w_down[0]
    block_rows = lax.all_gather(arrived, ("dp", "mp"), axis=1, tiled=True)
    row_count = block_rows.shape[1]
    base_rows = block_rows[0]
    tangent = block_rows[1 : probe_count + 1].reshape(probe_count * row_count, model_width)
    readout_rows = block_rows[probe_count + 1]
    gate_pre = jnp.dot(base_rows, gate_local, preferred_element_type=jnp.float32)
    up_pre = jnp.dot(base_rows, up_local, preferred_element_type=jnp.float32)
    readout = lax.dot_general(
        readout_rows, down_local, (((1,), (1,)), ((), ())), preferred_element_type=jnp.float32
    )
    gate_tan = jnp.dot(tangent, gate_local, preferred_element_type=jnp.float32).reshape(
        probe_count, row_count, -1
    )
    up_tan = jnp.dot(tangent, up_local, preferred_element_type=jnp.float32).reshape(
        probe_count, row_count, -1
    )
    first_slope, second_slope = silu_slopes(gate_pre)
    curved = second_slope * gate_tan * gate_tan * up_pre + 2.0 * first_slope * gate_tan * up_tan
    partial_quad = jnp.sum(curved * readout, axis=2)
    spread = partial_quad.reshape(probe_count, -1, experts, capacity)
    swapped = lax.all_to_all(spread, "expert", split_axis=2, concat_axis=2, tiled=True)
    returned_table = lax.psum_scatter(swapped, ("dp", "mp"), scatter_dimension=1, tiled=True)
    returned_table = returned_table.reshape(probe_count, experts * capacity)
    per_choice = jnp.dot(
        returned_table, placing.astype(jnp.float32).T, precision=lax.Precision.HIGHEST
    )
    return jnp.sum(per_choice.reshape(probe_count, tok_dev, top_count), axis=2)


class Layout:
    def __init__(self, mesh):
        self.dp = mesh.shape["dp"]
        self.expert = mesh.shape["expert"]
        self.core = 2
        self.y = mesh.shape["mp"] // self.core

    def pairs(self, dx, dz, dy, dc):
        out = []
        for x in range(self.dp):
            for z in range(self.expert):
                for y in range(self.y):
                    for c in range(self.core):
                        src = self.index(x, z, y, c)
                        dst = self.index(
                            (x + dx) % self.dp,
                            (z + dz) % self.expert,
                            (y + dy) % self.y,
                            (c + dc) % self.core,
                        )
                        out.append((src, dst))
        return out

    def index(self, x, z, y, c):
        return ((x * self.expert + z) * self.y + y) * self.core + c


AXES = ("dp", "expert", "mp")


def make_fast(lay):
    z_shifts = list(range(lay.expert))
    plane_shifts = [(dx, dy) for dx in range(lay.dp) for dy in range(lay.y)]

    def send(block, dx, dz, dy, dc):
        if dx == dz == dy == dc == 0:
            return block
        return lax.ppermute(block, AXES, lay.pairs(dx, dz, dy, dc))

    def over_z(block):
        return [send(block, 0, dz, 0, 0) for dz in z_shifts]

    def over_plane(block):
        return [send(block, dx, 0, dy, 0) for dx, dy in plane_shifts]

    def over_core(pieces):
        return [[send(piece, 0, 0, 0, dc) for piece in pieces] for dc in range(lay.core)]

    def join(pieces):
        return jnp.concatenate(pieces, axis=0)

    def pack(tokens, probes, cotangent, expert_ids, combine, cut):
        tok_dev, width = tokens.shape
        top = expert_ids.shape[1]

        def body(tok_ref, probe_ref, cot_ref, ids_ref, weight_ref, a_ref, b_ref):
            f32 = jnp.float32
            kinds = [tok_ref[...], *(probe_ref[p] for p in range(KINDS - 2)), cot_ref[...]]
            rows = jnp.concatenate([k.astype(f32) for k in kinds], axis=0).astype(jnp.bfloat16)
            a_ref[0, :, LANES:] = rows[:, :cut]
            b_ref[0] = rows[:, cut:]
            lane = lax.broadcasted_iota(jnp.int32, (tok_dev, LANES), 1)
            meta = jnp.zeros((tok_dev, LANES), f32)
            own = lax.broadcasted_iota(jnp.int32, (tok_dev, tok_dev), 0) == lax.broadcasted_iota(
                jnp.int32, (tok_dev, tok_dev), 1
            )

            def column(ref, k):
                return jnp.sum(jnp.where(own, ref[k : k + 1, :].astype(f32), 0.0), axis=1, keepdims=True)

            for k in range(top):
                rest = column(weight_ref, k)
                meta = jnp.where(lane == k, column(ids_ref, k), meta)
                for part in range(3):
                    value = rest.astype(jnp.bfloat16).astype(f32)
                    meta = jnp.where(lane == (part + 1) * top + k, value, meta)
                    rest = rest - value
            blank = jnp.zeros(((KINDS - 1) * tok_dev, LANES), f32)
            a_ref[0, :, :LANES] = jnp.concatenate([meta, blank], axis=0).astype(jnp.bfloat16)

        return pl.pallas_call(
            body,
            out_shape=(
                jax.ShapeDtypeStruct((1, KINDS * tok_dev, LANES + cut), jnp.bfloat16),
                jax.ShapeDtypeStruct((1, KINDS * tok_dev, width - cut), jnp.bfloat16),
            ),
            name="pack",
        )(tokens, probes, cotangent, expert_ids.T, combine.T)

    def on_device(tokens, probes, cotangent, expert_ids, combine, w_gate, w_up, w_down):
        return staged(tokens, probes, cotangent, expert_ids, combine, w_gate, w_up, w_down)

    def staged(tokens, probes, cotangent, expert_ids, combine, w_gate, w_up, w_down):
        tok_dev, width = tokens.shape
        probe_count = probes.shape[0]
        a, b = pack(tokens, probes, cotangent, expert_ids, combine, width * CUT // 32)
        a = join(over_z(a))
        b = join(over_plane(b))
        a = over_core(over_plane(a))
        b = over_core(over_z(b))
        partial = contract(a, b, w_gate[0], w_up[0], w_down[0], tok_dev, expert_ids.shape[1])
        swapped = lax.all_to_all(partial, AXES, split_axis=0, concat_axis=0, tiled=True)
        total = jnp.sum(swapped, axis=0)
        return total[: probe_count * tok_dev].reshape(probe_count, tok_dev)

    def contract(a, b, w_gate, w_up, w_down, tok_dev, top):
        width, ff = w_gate.shape
        tiles = ff // FF_TILE
        half = len(plane_shifts) * len(z_shifts)
        rows = 2 * half * tok_dev
        group = len(z_shifts)
        probe_count = KINDS - 2
        top_rows = (KINDS - 1) * rows
        size = group * tok_dev
        flat = [piece for core in a for piece in core] + [piece for core in b for piece in core]

        def body(*refs):
            refs = list(refs)
            pieces = [refs.pop(0) for _ in flat]
            wg, wu, wd, out_ref = [refs.pop(0) for _ in range(4)]
            lhs, gbuf, ubuf, dbuf, gate_ref, up_ref, read_ref, acc, sems = refs

            def copies(i, slot):
                at = pl.multiple_of(i * FF_TILE, FF_TILE)
                return (
                    pltpu.make_async_copy(wg.at[:, pl.ds(at, FF_TILE)], gbuf.at[slot], sems.at[0, slot]),
                    pltpu.make_async_copy(wu.at[:, pl.ds(at, FF_TILE)], ubuf.at[slot], sems.at[1, slot]),
                    pltpu.make_async_copy(wd.at[pl.ds(at, FF_TILE), :], dbuf.at[slot], sems.at[2, slot]),
                )

            for i in range(SLOTS):
                for c in copies(i, i):
                    c.start()

            def split(blocks, at, size):
                parts = [[] for _ in range(KINDS)]
                mask = lax.broadcasted_iota(jnp.int32, (8, size), 0) < tok_dev
                for (ra, ia), (rb, ib) in zip(blocks[::2], blocks[1::2]):
                    x = ra[ia, :, pl.ds(at, size)].astype(jnp.float32)
                    y = rb[ib, :, pl.ds(at, size)].astype(jnp.float32)
                    for h in range(2):
                        xh = x[8 * h : 8 * h + 8]
                        yh = y[8 * h : 8 * h + 8]
                        parts[2 * h].append(jnp.where(mask, xh, pltpu.roll(yh, tok_dev, 0)))
                        parts[2 * h + 1].append(jnp.where(mask, pltpu.roll(xh, tok_dev, 0), yh))
                return [jnp.concatenate(p, axis=0) for p in parts]

            expert = lax.axis_index("expert").astype(jnp.float32)
            count = len(plane_shifts)
            for core in range(lay.core):
                mine = pieces[core * count : (core + 1) * count]
                late = pieces[2 * count + core * group : 2 * count + (core + 1) * group]
                for j in range(count):
                    early = [(mine[j], dz) for dz in range(group)]
                    base = (core * count + j) * size
                    tags = split(early, 0, LANES)[0]
                    weight = jnp.zeros((size, 1), jnp.float32)
                    for k in range(top):
                        value = tags[:, top + k : top + k + 1] + tags[:, 2 * top + k : 2 * top + k + 1]
                        value = value + tags[:, 3 * top + k : 3 * top + k + 1]
                        weight = weight + jnp.where(tags[:, k : k + 1] == expert, value, 0.0)
                    wide = jnp.broadcast_to(weight, (size, COLUMNS))

                    def take(blocks, at, to):
                        parts = split(blocks, at, COLUMNS)
                        parts[-1] = wide * parts[-1]
                        for kind in range(KINDS):
                            lhs[pl.ds(kind * rows + base, size), pl.ds(to, COLUMNS)] = parts[kind].astype(jnp.bfloat16)

                    cut = mine[0].shape[2] - LANES
                    for k in range(cut // COLUMNS):
                        take(early, LANES + k * COLUMNS, k * COLUMNS)
                    for k in range((width - cut) // COLUMNS):
                        take([(late[dz], j) for dz in range(group)], k * COLUMNS, cut + k * COLUMNS)

            acc[...] = jnp.zeros(acc.shape, jnp.float32)

            def products(gate_w, up_w, down_w, slot):
                gate_ref[slot] = jnp.dot(lhs[:top_rows, :], gate_w, preferred_element_type=jnp.float32)
                up_ref[slot] = jnp.dot(lhs[:top_rows, :], up_w, preferred_element_type=jnp.float32)
                read_ref[slot] = lax.dot_general(
                    lhs[top_rows:, :], down_w, (((1,), (1,)), ((), ())), preferred_element_type=jnp.float32
                )

            def curve(slot):
                read = read_ref[slot]
                first, second = silu_slopes(gate_ref[slot, :rows])
                second = second * up_ref[slot, :rows] * read
                first = 2.0 * first * read
                for p in range(probe_count):
                    gate_tan = gate_ref[slot, pl.ds((p + 1) * rows, rows)]
                    up_tan = up_ref[slot, pl.ds((p + 1) * rows, rows)]
                    term = gate_tan * (second * gate_tan + first * up_tan)
                    for h in range(FF_TILE // LANES):
                        acc[p] += term[:, h * LANES : (h + 1) * LANES]

            def load(i):
                slot = lax.rem(i, SLOTS)
                for c in copies(i, slot):
                    c.wait()
                products(gbuf[slot], ubuf[slot], dbuf[slot], lax.rem(i, 2))

            def refill(i):
                @pl.when(i + SLOTS < tiles)
                def _():
                    for c in copies(i + SLOTS, lax.rem(i, SLOTS)):
                        c.start()

            load(0)
            refill(0)

            def tile(i, _):
                load(i)
                curve(lax.rem(i + 1, 2))
                refill(i)
                return 0

            lax.fori_loop(1, tiles, tile, 0)
            curve((tiles - 1) % 2)

            def device_of(block):
                x = lax.axis_index("dp")
                z = lax.axis_index("expert")
                m = lax.axis_index("mp")
                y = m // lay.core
                c = m % lay.core
                out = jnp.zeros(block.shape, jnp.int32)
                for dc in range(lay.core):
                    for j, (dx, dy) in enumerate(plane_shifts):
                        for dz in z_shifts:
                            src = lay.index(
                                (x + lay.dp - dx) % lay.dp,
                                (z + lay.expert - dz) % lay.expert,
                                (y + lay.y - dy) % lay.y,
                                (c + lay.core - dc) % lay.core,
                            )
                            out = jnp.where(block == dc * half + j * group + dz, src, out)
                return out

            block = lax.broadcasted_iota(jnp.int32, (8, rows), 1) // tok_dev
            source = device_of(block)[0:1]
            hot = source == lax.broadcasted_iota(jnp.int32, (2 * half, rows), 0)
            row = lax.broadcasted_iota(jnp.int32, (rows, LANES), 0) % tok_dev
            lane = lax.broadcasted_iota(jnp.int32, (rows, LANES), 1)
            spread = jnp.zeros((rows, LANES), jnp.float32)
            for p in range(probe_count):
                value = jnp.sum(acc[p], axis=1, keepdims=True)
                spread = spread + jnp.where(lane == row + p * tok_dev, value, 0.0)
            out_ref[...] = jnp.dot(
                hot.astype(jnp.float32), spread, precision=lax.Precision.HIGHEST, preferred_element_type=jnp.float32
            )

        vmem = pl.BlockSpec(memory_space=pltpu.VMEM)
        hbm = pl.BlockSpec(memory_space=pl.ANY)
        f32 = jnp.float32
        return pl.pallas_call(
            body,
            out_shape=jax.ShapeDtypeStruct((2 * half, LANES), f32),
            in_specs=[vmem] * len(flat) + [hbm] * 3,
            out_specs=vmem,
            scratch_shapes=[
                pltpu.VMEM((KINDS * rows, width), jnp.bfloat16),
                pltpu.VMEM((SLOTS, width, FF_TILE), jnp.bfloat16),
                pltpu.VMEM((SLOTS, width, FF_TILE), jnp.bfloat16),
                pltpu.VMEM((SLOTS, FF_TILE, width), jnp.bfloat16),
                pltpu.VMEM((2, top_rows, FF_TILE), f32),
                pltpu.VMEM((2, top_rows, FF_TILE), f32),
                pltpu.VMEM((2, rows, FF_TILE), f32),
                pltpu.VMEM((probe_count, rows, LANES), f32),
                pltpu.SemaphoreType.DMA((3, SLOTS)),
            ],
            compiler_params=pltpu.CompilerParams(vmem_limit_bytes=40 * 1024 * 1024),
            cost_estimate=pl.CostEstimate(
                flops=2 * (2 * top_rows + rows) * width * ff, bytes_accessed=3 * 2 * width * ff, transcendentals=0
            ),
            name="contract",
        )(*flat, w_gate, w_up, w_down)

    return on_device


def fits(mesh, args):
    tokens, probes, w_gate = args[0], args[1], args[5]
    rows = (probes.shape[0] + 2) * tokens.shape[0]
    tok_dev = tokens.shape[0] // mesh.size
    return (
        mesh.shape["mp"] % 2 == 0
        and w_gate.shape[0] == mesh.shape["expert"]
        and probes.shape[0] + 2 == KINDS
        and tok_dev == 4
        and 4 * rows * tokens.shape[1] <= VMEM_ROWS
        and w_gate.shape[2] % (mesh.shape["dp"] * mesh.shape["mp"] * FF_TILE) == 0
    )


def solution(mesh):
    in_specs = (
        P(("dp", "expert", "mp"), None),
        P(None, ("dp", "expert", "mp"), None),
        P(("dp", "expert", "mp"), None),
        P(("dp", "expert", "mp"), None),
        P(("dp", "expert", "mp"), None),
        P("expert", None, ("dp", "mp")),
        P("expert", None, ("dp", "mp")),
        P("expert", ("dp", "mp"), None),
    )
    out_specs = P(None, ("dp", "expert", "mp"))

    lay = Layout(mesh)

    def program(*args):
        if not fits(mesh, args):
            return jax.shard_map(
                routed_on_device, mesh=mesh, in_specs=in_specs, out_specs=out_specs, check_vma=False
            )(*args)
        step = jax.shard_map(make_fast(lay), mesh=mesh, in_specs=in_specs, out_specs=out_specs, check_vma=False)
        return step(*args)

    return program
```

```python
import jax
import jax.numpy as jnp
from jax import lax
from jax.experimental import pallas as pl
from jax.experimental.pallas import tpu as pltpu
from jax.sharding import PartitionSpec as P


LANES = 128
FF_TILE = 256
COLUMNS = 256
CUT = 24
SLOTS = 3
KINDS = 4
VMEM_ROWS = 16 * 1024 * 1024


def silu_slopes(preact):
    squash = jax.nn.sigmoid(preact)
    first_slope = squash * (1.0 + preact * (1.0 - squash))
    second_slope = squash * (1.0 - squash) * (2.0 + preact * (1.0 - 2.0 * squash))
    return (first_slope, second_slope)


def routed_on_device(tokens, probes, cotangent, expert_ids, combine, w_gate, w_up, w_down):
    tok_dev, model_width = tokens.shape
    probe_count = probes.shape[0]
    top_count = expert_ids.shape[1]
    experts = lax.axis_size("expert") * w_gate.shape[0]
    capacity = 2 * max(1, tok_dev * top_count // experts)
    routed = tok_dev * top_count
    flat_ids = expert_ids.reshape(routed)
    positions = jnp.arange(routed, dtype=jnp.int32)
    same_expert = flat_ids[:, None] == flat_ids[None, :]
    before = positions[None, :] < positions[:, None]
    slot_index = jnp.sum((same_expert & before).astype(jnp.int32), axis=1)
    expert_hot = flat_ids[:, None] == jnp.arange(experts, dtype=jnp.int32)[None, :]
    slot_hot = slot_index[:, None] == jnp.arange(capacity, dtype=jnp.int32)[None, :]
    placing = (expert_hot[:, :, None] & slot_hot[:, None, :]).reshape(routed, experts * capacity)
    scaled = (
        combine.reshape(routed, 1) * jnp.repeat(cotangent.astype(jnp.float32), top_count, axis=0)
    ).astype(jnp.bfloat16)
    stacked = jnp.repeat(jnp.concatenate([tokens[None], probes], axis=0), top_count, axis=1)
    stacked = jnp.concatenate([stacked, scaled[None]], axis=0)
    outgoing = jnp.einsum(
        "nk,rnd->rkd", placing.astype(jnp.bfloat16), stacked, preferred_element_type=jnp.float32
    ).astype(jnp.bfloat16)
    outgoing = outgoing.reshape(probe_count + 2, experts, capacity, model_width)
    arrived = lax.all_to_all(outgoing, "expert", split_axis=1, concat_axis=1, tiled=True)
    arrived = arrived.reshape(probe_count + 2, experts * capacity, model_width)
    gate_local = w_gate[0]
    up_local = w_up[0]
    down_local = w_down[0]
    block_rows = lax.all_gather(arrived, ("dp", "mp"), axis=1, tiled=True)
    row_count = block_rows.shape[1]
    base_rows = block_rows[0]
    tangent = block_rows[1 : probe_count + 1].reshape(probe_count * row_count, model_width)
    readout_rows = block_rows[probe_count + 1]
    gate_pre = jnp.dot(base_rows, gate_local, preferred_element_type=jnp.float32)
    up_pre = jnp.dot(base_rows, up_local, preferred_element_type=jnp.float32)
    readout = lax.dot_general(
        readout_rows, down_local, (((1,), (1,)), ((), ())), preferred_element_type=jnp.float32
    )
    gate_tan = jnp.dot(tangent, gate_local, preferred_element_type=jnp.float32).reshape(
        probe_count, row_count, -1
    )
    up_tan = jnp.dot(tangent, up_local, preferred_element_type=jnp.float32).reshape(
        probe_count, row_count, -1
    )
    first_slope, second_slope = silu_slopes(gate_pre)
    curved = second_slope * gate_tan * gate_tan * up_pre + 2.0 * first_slope * gate_tan * up_tan
    partial_quad = jnp.sum(curved * readout, axis=2)
    spread = partial_quad.reshape(probe_count, -1, experts, capacity)
    swapped = lax.all_to_all(spread, "expert", split_axis=2, concat_axis=2, tiled=True)
    returned_table = lax.psum_scatter(swapped, ("dp", "mp"), scatter_dimension=1, tiled=True)
    returned_table = returned_table.reshape(probe_count, experts * capacity)
    per_choice = jnp.dot(
        returned_table, placing.astype(jnp.float32).T, precision=lax.Precision.HIGHEST
    )
    return jnp.sum(per_choice.reshape(probe_count, tok_dev, top_count), axis=2)


class Layout:
    def __init__(self, mesh):
        self.dp = mesh.shape["dp"]
        self.expert = mesh.shape["expert"]
        self.core = 2
        self.y = mesh.shape["mp"] // self.core

    def pairs(self, dx, dz, dy, dc):
        out = []
        for x in range(self.dp):
            for z in range(self.expert):
                for y in range(self.y):
                    for c in range(self.core):
                        src = self.index(x, z, y, c)
                        dst = self.index(
                            (x + dx) % self.dp,
                            (z + dz) % self.expert,
                            (y + dy) % self.y,
                            (c + dc) % self.core,
                        )
                        out.append((src, dst))
        return out

    def index(self, x, z, y, c):
        return ((x * self.expert + z) * self.y + y) * self.core + c


AXES = ("dp", "expert", "mp")


def make_fast(lay):
    z_shifts = list(range(lay.expert))
    plane_shifts = [(dx, dy) for dx in range(lay.dp) for dy in range(lay.y)]

    def send(block, dx, dz, dy, dc):
        if dx == dz == dy == dc == 0:
            return block
        return lax.ppermute(block, AXES, lay.pairs(dx, dz, dy, dc))

    def over_z(block):
        return [send(block, 0, dz, 0, 0) for dz in z_shifts]

    def over_plane(block):
        return [send(block, dx, 0, dy, 0) for dx, dy in plane_shifts]

    def over_core(pieces):
        return [[send(piece, 0, 0, 0, dc) for piece in pieces] for dc in range(lay.core)]

    def join(pieces):
        return jnp.concatenate(pieces, axis=0)

    def pack(tokens, probes, cotangent, expert_ids, combine, cut):
        tok_dev, width = tokens.shape
        top = expert_ids.shape[1]

        def body(tok_ref, probe_ref, cot_ref, ids_ref, weight_ref, a_ref, b_ref):
            f32 = jnp.float32
            kinds = [tok_ref[...], *(probe_ref[p] for p in range(KINDS - 2)), cot_ref[...]]
            rows = jnp.concatenate([k.astype(f32) for k in kinds], axis=0).astype(jnp.bfloat16)
            a_ref[0, :, LANES:] = rows[:, :cut]
            b_ref[0] = rows[:, cut:]
            lane = lax.broadcasted_iota(jnp.int32, (tok_dev, LANES), 1)
            meta = jnp.zeros((tok_dev, LANES), f32)
            own = lax.broadcasted_iota(jnp.int32, (tok_dev, tok_dev), 0) == lax.broadcasted_iota(
                jnp.int32, (tok_dev, tok_dev), 1
            )

            def column(ref, k):
                return jnp.sum(jnp.where(own, ref[k : k + 1, :].astype(f32), 0.0), axis=1, keepdims=True)

            for k in range(top):
                rest = column(weight_ref, k)
                meta = jnp.where(lane == k, column(ids_ref, k), meta)
                for part in range(3):
                    value = rest.astype(jnp.bfloat16).astype(f32)
                    meta = jnp.where(lane == (part + 1) * top + k, value, meta)
                    rest = rest - value
            blank = jnp.zeros(((KINDS - 1) * tok_dev, LANES), f32)
            a_ref[0, :, :LANES] = jnp.concatenate([meta, blank], axis=0).astype(jnp.bfloat16)

        return pl.pallas_call(
            body,
            out_shape=(
                jax.ShapeDtypeStruct((1, KINDS * tok_dev, LANES + cut), jnp.bfloat16),
                jax.ShapeDtypeStruct((1, KINDS * tok_dev, width - cut), jnp.bfloat16),
            ),
            name="pack",
        )(tokens, probes, cotangent, expert_ids.T, combine.T)

    def on_device(tokens, probes, cotangent, expert_ids, combine, w_gate, w_up, w_down):
        return staged(tokens, probes, cotangent, expert_ids, combine, w_gate, w_up, w_down)

    def staged(tokens, probes, cotangent, expert_ids, combine, w_gate, w_up, w_down):
        tok_dev, width = tokens.shape
        probe_count = probes.shape[0]
        a, b = pack(tokens, probes, cotangent, expert_ids, combine, width * CUT // 32)
        a = over_z(a)
        b = join(over_plane(b))
        middle = LANES + (a[0].shape[2] - LANES) // 2
        low = join([p[:, :, :middle] for p in a])
        high = join([p[:, :, middle:] for p in a])
        low_x = send(low, 1, 0, 0, 0)
        high_y = send(high, 0, 0, 1, 0)
        high_x = send(high, 1, 0, 0, 0)
        low_y = send(low, 0, 0, 1, 0)
        low_far = send(low_x, 0, 0, 1, 0)
        high_far = send(high_y, 1, 0, 0, 0)
        a = [low, high, low_y, high_y, low_x, high_x, low_far, high_far]
        a = over_core(a)
        b = over_core(over_z(b))
        partial = contract(a, b, w_gate[0], w_up[0], w_down[0], tok_dev, expert_ids.shape[1])
        swapped = lax.all_to_all(partial, AXES, split_axis=0, concat_axis=0, tiled=True)
        total = jnp.sum(swapped, axis=0)
        return total[: probe_count * tok_dev].reshape(probe_count, tok_dev)

    def contract(a, b, w_gate, w_up, w_down, tok_dev, top):
        width, ff = w_gate.shape
        tiles = ff // FF_TILE
        half = len(plane_shifts) * len(z_shifts)
        rows = 2 * half * tok_dev
        group = len(z_shifts)
        probe_count = KINDS - 2
        top_rows = (KINDS - 1) * rows
        size = group * tok_dev
        flat = [piece for core in a for piece in core] + [piece for core in b for piece in core]

        def body(*refs):
            refs = list(refs)
            pieces = [refs.pop(0) for _ in flat]
            wg, wu, wd, out_ref = [refs.pop(0) for _ in range(4)]
            lhs, gbuf, ubuf, dbuf, gate_ref, up_ref, read_ref, acc, sems = refs

            def copies(i, slot):
                at = pl.multiple_of(i * FF_TILE, FF_TILE)
                return (
                    pltpu.make_async_copy(wg.at[:, pl.ds(at, FF_TILE)], gbuf.at[slot], sems.at[0, slot]),
                    pltpu.make_async_copy(wu.at[:, pl.ds(at, FF_TILE)], ubuf.at[slot], sems.at[1, slot]),
                    pltpu.make_async_copy(wd.at[pl.ds(at, FF_TILE), :], dbuf.at[slot], sems.at[2, slot]),
                )

            for i in range(SLOTS):
                for c in copies(i, i):
                    c.start()

            def split(blocks, at, size):
                parts = [[] for _ in range(KINDS)]
                mask = lax.broadcasted_iota(jnp.int32, (8, size), 0) < tok_dev
                for (ra, ia), (rb, ib) in zip(blocks[::2], blocks[1::2]):
                    x = ra[ia, :, pl.ds(at, size)].astype(jnp.float32)
                    y = rb[ib, :, pl.ds(at, size)].astype(jnp.float32)
                    for h in range(2):
                        xh = x[8 * h : 8 * h + 8]
                        yh = y[8 * h : 8 * h + 8]
                        parts[2 * h].append(jnp.where(mask, xh, pltpu.roll(yh, tok_dev, 0)))
                        parts[2 * h + 1].append(jnp.where(mask, pltpu.roll(xh, tok_dev, 0), yh))
                return [jnp.concatenate(p, axis=0) for p in parts]

            expert = lax.axis_index("expert").astype(jnp.float32)
            count = len(plane_shifts)
            for core in range(lay.core):
                mine = pieces[core * 2 * count : (core + 1) * 2 * count]
                late = pieces[4 * count + core * group : 4 * count + (core + 1) * group]
                for j in range(count):
                    early = [(mine[2 * j], dz) for dz in range(group)]
                    next_half = [(mine[2 * j + 1], dz) for dz in range(group)]
                    base = (core * count + j) * size
                    tags = split(early, 0, LANES)[0]
                    weight = jnp.zeros((size, 1), jnp.float32)
                    for k in range(top):
                        value = tags[:, top + k : top + k + 1] + tags[:, 2 * top + k : 2 * top + k + 1]
                        value = value + tags[:, 3 * top + k : 3 * top + k + 1]
                        weight = weight + jnp.where(tags[:, k : k + 1] == expert, value, 0.0)
                    wide = jnp.broadcast_to(weight, (size, COLUMNS))

                    def take(blocks, at, to):
                        parts = split(blocks, at, COLUMNS)
                        parts[-1] = wide * parts[-1]
                        for kind in range(KINDS):
                            lhs[pl.ds(kind * rows + base, size), pl.ds(to, COLUMNS)] = parts[kind].astype(jnp.bfloat16)

                    part = mine[1].shape[2]
                    cut = 2 * part
                    for k in range(part // COLUMNS):
                        take(early, LANES + k * COLUMNS, k * COLUMNS)
                    for k in range(part // COLUMNS):
                        take(next_half, k * COLUMNS, part + k * COLUMNS)
                    for k in range((width - cut) // COLUMNS):
                        take([(late[dz], j) for dz in range(group)], k * COLUMNS, cut + k * COLUMNS)

            acc[...] = jnp.zeros(acc.shape, jnp.float32)

            def products(gate_w, up_w, down_w, slot):
                gate_ref[slot] = jnp.dot(lhs[:top_rows, :], gate_w, preferred_element_type=jnp.float32)
                up_ref[slot] = jnp.dot(lhs[:top_rows, :], up_w, preferred_element_type=jnp.float32)
                read_ref[slot] = lax.dot_general(
                    lhs[top_rows:, :], down_w, (((1,), (1,)), ((), ())), preferred_element_type=jnp.float32
                )

            def curve(slot):
                read = read_ref[slot]
                first, second = silu_slopes(gate_ref[slot, :rows])
                second = second * up_ref[slot, :rows] * read
                first = 2.0 * first * read
                for p in range(probe_count):
                    gate_tan = gate_ref[slot, pl.ds((p + 1) * rows, rows)]
                    up_tan = up_ref[slot, pl.ds((p + 1) * rows, rows)]
                    term = gate_tan * (second * gate_tan + first * up_tan)
                    for h in range(FF_TILE // LANES):
                        acc[p] += term[:, h * LANES : (h + 1) * LANES]

            def load(i):
                slot = lax.rem(i, SLOTS)
                for c in copies(i, slot):
                    c.wait()
                products(gbuf[slot], ubuf[slot], dbuf[slot], lax.rem(i, 2))

            def refill(i):
                @pl.when(i + SLOTS < tiles)
                def _():
                    for c in copies(i + SLOTS, lax.rem(i, SLOTS)):
                        c.start()

            load(0)
            refill(0)

            def tile(i, _):
                load(i)
                curve(lax.rem(i + 1, 2))
                refill(i)
                return 0

            lax.fori_loop(1, tiles, tile, 0)
            curve((tiles - 1) % 2)

            def device_of(block):
                x = lax.axis_index("dp")
                z = lax.axis_index("expert")
                m = lax.axis_index("mp")
                y = m // lay.core
                c = m % lay.core
                out = jnp.zeros(block.shape, jnp.int32)
                for dc in range(lay.core):
                    for j, (dx, dy) in enumerate(plane_shifts):
                        for dz in z_shifts:
                            src = lay.index(
                                (x + lay.dp - dx) % lay.dp,
                                (z + lay.expert - dz) % lay.expert,
                                (y + lay.y - dy) % lay.y,
                                (c + lay.core - dc) % lay.core,
                            )
                            out = jnp.where(block == dc * half + j * group + dz, src, out)
                return out

            block = lax.broadcasted_iota(jnp.int32, (8, rows), 1) // tok_dev
            source = device_of(block)[0:1]
            hot = source == lax.broadcasted_iota(jnp.int32, (2 * half, rows), 0)
            row = lax.broadcasted_iota(jnp.int32, (rows, LANES), 0) % tok_dev
            lane = lax.broadcasted_iota(jnp.int32, (rows, LANES), 1)
            spread = jnp.zeros((rows, LANES), jnp.float32)
            for p in range(probe_count):
                value = jnp.sum(acc[p], axis=1, keepdims=True)
                spread = spread + jnp.where(lane == row + p * tok_dev, value, 0.0)
            out_ref[...] = jnp.dot(
                hot.astype(jnp.float32), spread, precision=lax.Precision.HIGHEST, preferred_element_type=jnp.float32
            )

        vmem = pl.BlockSpec(memory_space=pltpu.VMEM)
        hbm = pl.BlockSpec(memory_space=pl.ANY)
        f32 = jnp.float32
        return pl.pallas_call(
            body,
            out_shape=jax.ShapeDtypeStruct((2 * half, LANES), f32),
            in_specs=[vmem] * len(flat) + [hbm] * 3,
            out_specs=vmem,
            scratch_shapes=[
                pltpu.VMEM((KINDS * rows, width), jnp.bfloat16),
                pltpu.VMEM((SLOTS, width, FF_TILE), jnp.bfloat16),
                pltpu.VMEM((SLOTS, width, FF_TILE), jnp.bfloat16),
                pltpu.VMEM((SLOTS, FF_TILE, width), jnp.bfloat16),
                pltpu.VMEM((2, top_rows, FF_TILE), f32),
                pltpu.VMEM((2, top_rows, FF_TILE), f32),
                pltpu.VMEM((2, rows, FF_TILE), f32),
                pltpu.VMEM((probe_count, rows, LANES), f32),
                pltpu.SemaphoreType.DMA((3, SLOTS)),
            ],
            compiler_params=pltpu.CompilerParams(vmem_limit_bytes=40 * 1024 * 1024),
            cost_estimate=pl.CostEstimate(
                flops=2 * (2 * top_rows + rows) * width * ff, bytes_accessed=3 * 2 * width * ff, transcendentals=0
            ),
            name="contract",
        )(*flat, w_gate, w_up, w_down)

    return on_device


def fits(mesh, args):
    tokens, probes, w_gate = args[0], args[1], args[5]
    rows = (probes.shape[0] + 2) * tokens.shape[0]
    tok_dev = tokens.shape[0] // mesh.size
    return (
        mesh.shape["mp"] == 4
        and mesh.shape["dp"] == 2
        and w_gate.shape[0] == mesh.shape["expert"]
        and probes.shape[0] + 2 == KINDS
        and tok_dev == 4
        and 4 * rows * tokens.shape[1] <= VMEM_ROWS
        and w_gate.shape[2] % (mesh.shape["dp"] * mesh.shape["mp"] * FF_TILE) == 0
    )


def solution(mesh):
    in_specs = (
        P(("dp", "expert", "mp"), None),
        P(None, ("dp", "expert", "mp"), None),
        P(("dp", "expert", "mp"), None),
        P(("dp", "expert", "mp"), None),
        P(("dp", "expert", "mp"), None),
        P("expert", None, ("dp", "mp")),
        P("expert", None, ("dp", "mp")),
        P("expert", ("dp", "mp"), None),
    )
    out_specs = P(None, ("dp", "expert", "mp"))

    lay = Layout(mesh)

    def program(*args):
        if not fits(mesh, args):
            return jax.shard_map(
                routed_on_device, mesh=mesh, in_specs=in_specs, out_specs=out_specs, check_vma=False
            )(*args)
        step = jax.shard_map(make_fast(lay), mesh=mesh, in_specs=in_specs, out_specs=out_specs, check_vma=False)
        return step(*args)

    return program
```
